768 devices in a mesh: gx: 96 (over z_lo, y, core), gy: 2 (over z_hi), gz: 4 (over x).
Axes of the slice: x: 4, y: 8, z: 12 (z_hi: 2, z_lo: 6; z = z_hi * 6 + z_lo), core: 2. Of those that a mesh axis runs over, the one named last changes fastest.
Arguments:
- adjoint_in: float32 [19, 768, 16, 512], P(None, 'gx', 'gy', 'gz'), may hold values from -16 to 16
- forward_states: float32 [2, 19, 768, 16, 512], P(None, None, 'gx', 'gy', 'gz'), may hold values from 0.01 to 0.63
- design: float32 [768, 16, 512], P('gx', 'gy', 'gz'), may hold values from 0 to 1
- solid_mask: int32 [768, 16, 512], P('gx', 'gy', 'gz'), may hold values 0 or 1
- boundary_kind: int32 [768, 16, 512], P('gx', 'gy', 'gz'), may hold values from 0 to 2, as said below
Outputs:
- adjoint_out: float32 [19, 768, 16, 512], P(None, 'gx', 'gy', 'gz')
- sensitivity: float32 [768, 16, 512], P('gx', 'gy', 'gz')
- objective: float32 [], replicated
- sens_rms: float32 [], replicated
The draws below stay inside these ranges and needn't reach their ends.
Inputs may be any that keep to these rules, and one draw needn't show every extreme that they name: `boundary_kind`: 1 marks inlet cells, 2 outlet cells.
All inputs are finite; a program needn't handle non-finite values. No bound on the sum of `solid_mask` on one device may be relied on, other than what follows from the above.
Results may differ from the reference program's by a relative error of at most 0.0003.
Values sent between devices are 32-bit elements; how exact they have to be, the bound alone decides.
A program may use at most 32 MiB of HBM per device.

```python
import jax
import jax.numpy as jnp
import numpy as np
from jax import lax

CX = 8
NX = 768
NY = 16
NZ = 512


stream_sign = np.array([0, 1, -1, 0, 0, 0, 0, 1, -1, 1, -1, 1, -1, 1, -1, 0, 0, 0, 0], dtype=np.float32)


lattice_weights = np.array([1.0 / 3] + [1.0 / 18] * 6 + [1.0 / 36] * 12, dtype=np.float32)


def draw_adjoint_in(key, part):
    xpos = jnp.arange(NX).astype(jnp.float32) / (NX - 1)
    values = jnp.clip(jax.random.normal(key, (19, NX, NY, NZ), jnp.float32), -4.0, 4.0)
    ramp = 1.0 + 2.0 * xpos
    return (values * ramp[None, :, None, None]).astype(jnp.float32)


def draw_forward_states(key, part):
    values = jnp.clip(jax.random.normal(key, (2, 19, NX, NY, NZ), jnp.float32), -2.5, 2.5)
    flow = 0.05
    scale = lattice_weights * (1.0 + 3.0 * flow * stream_sign)
    return (scale[None, :, None, None, None] * jnp.exp(0.25 * values)).astype(jnp.float32)


def draw_boundary_kind(key, part):
    picks = jax.random.randint(key, (NX, NY, NZ), 0, 32)
    return jnp.where(picks == 0, 1, jnp.where(picks == 1, 2, 0)).astype(jnp.int32)


def set_ends(values, stream_key, smallest, top_value):
    dims = values.shape
    place = [jax.random.randint(jax.random.fold_in(stream_key, axis), (), 0, dims[axis]) for axis in range(len(dims))]
    values = values.at[tuple(place)].set(smallest)
    longest = dims.index(max(dims))
    place[longest] = (place[longest] + 1) % dims[longest]
    return values.at[tuple(place)].set(top_value)


def shard_levels(key, extent, cuts, smallest, largest):
    factor_of, own = 1.0, jax.random.fold_in(key, 6)
    for position, shards_of in cuts:
        heights = jnp.exp(jax.random.uniform(jax.random.fold_in(own, position), (shards_of,), jnp.float32, smallest / len(cuts), largest / len(cuts)))
        factor_of = factor_of * jnp.repeat(heights, extent[position] // shards_of).reshape([-1 if axis == position else 1 for axis in range(len(extent))])
    return factor_of


def setup_inputs(seed: int = 0) -> dict:
    key_of = jax.random.split(jax.random.key(seed), 6)
    return {
        "adjoint_in": draw_adjoint_in(jax.random.fold_in(key_of[5], 71), 0),
        "forward_states": draw_forward_states(jax.random.fold_in(key_of[5], 71), 0),
        "design": jnp.clip(1.0 * jax.random.uniform(key_of[2], (NX, NY, NZ), jnp.float32) ** shard_levels(key_of[2], (NX, NY, NZ), ((0, 96), (1, 2), (2, 4)), -0.2, 0.2), 0.0, 1.0),
        "solid_mask": set_ends((jax.random.randint(key_of[3], (NX, NY, NZ), 0, 8) < 1).astype(jnp.int32), jax.random.fold_in(key_of[3], 1), 0, 1),
        "boundary_kind": draw_boundary_kind(jax.random.fold_in(key_of[5], 71), 0),
    }


lattice_table = np.array([[0, 0, 0], [1, 0, 0], [-1, 0, 0], [0, 1, 0], [0, -1, 0], [0, 0, 1], [0, 0, -1], [1, 1, 0], [-1, -1, 0], [1, -1, 0], [-1, 1, 0], [1, 0, 1], [-1, 0, -1], [1, 0, -1], [-1, 0, 1], [0, 1, 1], [0, -1, -1], [0, 1, -1], [0, -1, 1]], dtype=np.int32)
velocity_table = np.array(lattice_table, dtype=np.float32)
lattice_weights = np.array([1.0 / 3] + [1.0 / 18] * 6 + [1.0 / 36] * 12, dtype=np.float32)
opposite_index = [0, 2, 1, 4, 3, 6, 5, 8, 7, 10, 9, 12, 11, 14, 13, 16, 15, 18, 17]
brinkman_max = 4.0
convexity = 0.1
inflow_speed = 0.08

def build_relax(lattice):
    cx = lattice[:, 0].astype(np.float32)
    cy = lattice[:, 1].astype(np.float32)
    cz = lattice[:, 2].astype(np.float32)
    csq = cx * cx + cy * cy + cz * cz
    rows = [np.ones(19, dtype=np.float32), 19 * csq - 30, (21 * csq * csq - 53 * csq + 24) / 2, cx, (5 * csq - 9) * cx, cy, (5 * csq - 9) * cy, cz, (5 * csq - 9) * cz, 3 * cx * cx - csq, (3 * csq - 5) * (3 * cx * cx - csq), cy * cy - cz * cz, (3 * csq - 5) * (cy * cy - cz * cz), cx * cy, cy * cz, cx * cz, (cy * cy - cz * cz) * cx, (cz * cz - cx * cx) * cy, (cx * cx - cy * cy) * cz]
    moments = np.stack(rows).astype(np.float32)
    shear = 1.0 / 0.6
    rates = np.array([0, 1.19, 1.4, 0, 1.2, 0, 1.2, 0, 1.2, shear, 1.4, shear, 1.4, shear, shear, shear, 1.98, 1.98, 1.98], dtype=np.float32)
    norms = np.sum(moments * moments, axis=1)
    scaled = moments.T * (rates / norms)[None, :]
    return (scaled @ moments).astype(np.float32)

def equilibrium(density, velocity):
    projected = jnp.tensordot(velocity_table, velocity, axes=(1, 0), precision=lax.Precision.HIGHEST)
    squared = lax.optimization_barrier(jnp.sum(velocity * velocity, axis=0))
    return lattice_weights[:, None, None, None] * density * (1.0 + 3.0 * projected + 4.5 * projected * projected - 1.5 * squared)

def post_and_cost(dist, design, solid, kind, weight):
    relax_matrix = build_relax(lattice_table)
    density = lax.optimization_barrier(jnp.sum(dist, axis=0))
    flux = jnp.tensordot(velocity_table.T, dist, axes=(1, 0), precision=lax.Precision.HIGHEST)
    damping = 1.0 / (1.0 + brinkman_max * convexity * (1.0 - design) / (convexity + design))
    velocity = flux / density * damping
    collided = dist - jnp.tensordot(relax_matrix, dist - equilibrium(density, velocity), axes=(1, 0), precision=lax.Precision.HIGHEST)
    ones = jnp.ones_like(density)
    inflow = equilibrium(density, jnp.stack([inflow_speed * ones, 0.0 * ones, 0.0 * ones]))
    outflow = equilibrium(ones, velocity)
    bounced = jnp.stack([dist[k] for k in opposite_index])
    post = jnp.where(solid == 1, bounced, jnp.where(kind == 1, inflow, jnp.where(kind == 2, outflow, collided)))
    fluid = (solid == 0).astype(jnp.float32)
    cost = weight * fluid * 0.5 * density * lax.optimization_barrier(jnp.sum(velocity * velocity, axis=0))
    return (post, cost)

def adjoint_step(dist, design, solid, kind, weight, pulled):

    def local(d, g):
        return post_and_cost(d, g, solid, kind, weight)
    outs, backward = jax.vjp(local, dist, design)
    new_adjoint, sens = backward((pulled, jnp.ones_like(outs[1])))
    return (new_adjoint, sens, jnp.sum(outs[1]))

def pull_back(adjoint):
    length_x, length_y, length_z = adjoint.shape[1:]
    padded = jnp.pad(adjoint, ((0, 0), (1, 1), (1, 1), (1, 1)))
    pieces = []
    for i in range(19):
        cx, cy, cz = (int(lattice_table[i, 0]), int(lattice_table[i, 1]), int(lattice_table[i, 2]))
        pieces.append(padded[i, 1 + cx:1 + cx + length_x, 1 + cy:1 + cy + length_y, 1 + cz:1 + cz + length_z])
    return jnp.stack(pieces)

def reference(adjoint_in, forward_states, design, solid_mask, boundary_kind):
    xpos = jnp.arange(NX, dtype=jnp.int32).astype(jnp.float32)
    weight = (1.0 + 2.0 * xpos / (NX - 1))[:, None, None]
    blocks = NX // CX
    adjoint = adjoint_in
    sens_total = jnp.zeros((NX, NY, NZ), jnp.float32)
    cost_total = jnp.zeros((), jnp.float32)
    for t in (1, 0):
        pulled = pull_back(adjoint)
        state = forward_states[t]

        def block_step(b):
            start = (b * CX).astype(jnp.int32)
            return adjoint_step(lax.dynamic_slice_in_dim(state, start, CX, 1), lax.dynamic_slice_in_dim(design, start, CX, 0), lax.dynamic_slice_in_dim(solid_mask, start, CX, 0), lax.dynamic_slice_in_dim(boundary_kind, start, CX, 0), lax.dynamic_slice_in_dim(weight, start, CX, 0), lax.dynamic_slice_in_dim(pulled, start, CX, 1))
        new_blocks, sens_blocks, cost_blocks = lax.map(block_step, jnp.arange(blocks, dtype=jnp.int32))
        adjoint = jnp.transpose(new_blocks, (1, 0, 2, 3, 4)).reshape(19, NX, NY, NZ)
        sens_total = sens_total + sens_blocks.reshape(NX, NY, NZ)
        cost_total = cost_total + jnp.sum(cost_blocks)
    cells = NX * NY * NZ
    objective = cost_total / cells
    sens_rms = jnp.sqrt(jnp.sum(sens_total * sens_total) / cells + 1e-06)
    return (adjoint, sens_total / sens_rms, objective, sens_rms)
```

```python
import functools

import jax
import jax.numpy as jnp
import numpy as np
from jax import lax
from jax.experimental import pallas as pl
from jax.experimental.pallas import tpu as pltpu
from jax.sharding import Mesh
from jax.sharding import PartitionSpec as P

AXES = ("gx_0", "gx_1", "gx_2", "gy", "gz")
GX = AXES[:3]
MESH = pl.DeviceIdType.MESH
f32 = jnp.float32

lattice = np.array(
    [
        [0, 0, 0],
        [1, 0, 0],
        [-1, 0, 0],
        [0, 1, 0],
        [0, -1, 0],
        [0, 0, 1],
        [0, 0, -1],
        [1, 1, 0],
        [-1, -1, 0],
        [1, -1, 0],
        [-1, 1, 0],
        [1, 0, 1],
        [-1, 0, -1],
        [1, 0, -1],
        [-1, 0, 1],
        [0, 1, 1],
        [0, -1, -1],
        [0, 1, -1],
        [0, -1, 1],
    ],
    dtype=np.int32,
)
X_PLUS, X_MINUS = [1, 7, 9, 11, 13], [2, 8, 10, 12, 14]
Y_PLUS, Y_MINUS = [3, 7, 10, 15, 17], [4, 9, 8, 18, 16]
Z_PLUS, Z_MINUS = [5, 11, 14, 15, 18], [6, 12, 13, 16, 17]
MESSAGES = (
    ("xd", (-1, 0, 0)),
    ("xu", (1, 0, 0)),
    ("zd", (0, 0, -1)),
    ("zu", (0, 0, 1)),
    ("dd", (-1, 0, -1)),
    ("uu", (1, 0, 1)),
    ("du", (-1, 0, 1)),
    ("ud", (1, 0, -1)),
    ("f", (0, 1, 0)),
    ("fxd", (-1, 1, 0)),
    ("fxu", (1, 1, 0)),
    ("fzd", (0, 1, -1)),
    ("fzu", (0, 1, 1)),
)
NEAR = range(8)
FAR = range(8, 13)


def moment_scales():
    c = lattice.astype(np.float64)
    cx, cy, cz = c[:, 0], c[:, 1], c[:, 2]
    q = cx * cx + cy * cy + cz * cz
    rows = np.stack(
        [
            np.ones(19),
            19 * q - 30,
            (21 * q * q - 53 * q + 24) / 2,
            cx,
            (5 * q - 9) * cx,
            cy,
            (5 * q - 9) * cy,
            cz,
            (5 * q - 9) * cz,
            3 * cx * cx - q,
            (3 * q - 5) * (3 * cx * cx - q),
            cy * cy - cz * cz,
            (3 * q - 5) * (cy * cy - cz * cz),
            cx * cy,
            cy * cz,
            cx * cz,
            (cy * cy - cz * cz) * cx,
            (cz * cz - cx * cx) * cy,
            (cx * cx - cy * cy) * cz,
        ]
    )
    shear = 1.0 / 0.6
    rates = np.array(
        [0, 1.19, 1.4, 0, 1.2, 0, 1.2, 0, 1.2, shear, 1.4, shear, 1.4]
        + [shear] * 3
        + [1.98] * 3
    )
    return [float(v) for v in rates / np.sum(rows * rows, axis=1)]


SCALE = moment_scales()


def step_tile(q, co):
    s = {i: q[i] + q[i + 1] for i in range(1, 19, 2)}
    d = {i: q[i] - q[i + 1] for i in range(1, 19, 2)}
    exy, exz, eyz = s[7] + s[9], s[11] + s[13], s[15] + s[17]
    mxy, mxz, myz = s[7] - s[9], s[11] - s[13], s[15] - s[17]
    sax = s[1] + s[3] + s[5]
    exa = exy + exz
    sed = exa + eyz
    dxy, exy_y = d[7] + d[9], d[7] - d[9]
    dxz, exz_z = d[11] + d[13], d[11] - d[13]
    dyz, eyz_z = d[15] + d[17], d[15] - d[17]
    dx, dy, dz = dxy + dxz, exy_y + dyz, exz_z + eyz_z
    k = SCALE
    t1 = k[1] * (8.0 * sed - 11.0 * sax - 30.0 * q[0])
    t2 = k[2] * (sed - 4.0 * sax + 12.0 * q[0])
    t4 = k[4] * (dx - 4.0 * d[1])
    t6 = k[6] * (dy - 4.0 * d[3])
    t8 = k[8] * (dz - 4.0 * d[5])
    aniso = 3.0 * s[1] - sax
    edges = sed - 3.0 * eyz
    t9 = k[9] * (aniso + edges)
    t10 = k[10] * (edges - 2.0 * aniso)
    yz = s[3] - s[5]
    exyz = exy - exz
    t11 = k[11] * (yz + exyz)
    t12 = k[12] * (exyz - 2.0 * yz)
    t13, t14, t15 = k[13] * mxy, k[14] * myz, k[15] * mxz
    t16 = k[16] * (dxy - dxz)
    t17 = k[17] * (dyz - exy_y)
    t18 = k[18] * (exz_z - eyz_z)
    raw = co["raw"] != 0.0

    def pick(a, b):
        return jnp.where(raw, a, b)

    w0, w1, w2 = 1.0 / 3.0, 1.0 / 18.0, 1.0 / 36.0
    iso = (5.0 / 9.0) * t1 - (2.0 / 9.0) * t2
    yza = (1.0 / 9.0) * t10 - (2.0 / 9.0) * t9
    yzb = (2.0 / 9.0) * t11 - (1.0 / 9.0) * t12
    s0 = pick(w0 * q[0] + w1 * sax + w2 * sed, 3.0 * t2 - 11.0 * t1)
    s1x = pick(w1 * d[1] + w2 * dx, (-2.0 / 9.0) * t4)
    s1y = pick(w1 * d[3] + w2 * dy, (-2.0 / 9.0) * t6)
    s1z = pick(w1 * d[5] + w2 * dz, (-2.0 / 9.0) * t8)
    sxx = pick(w1 * s[1] + w2 * exa, iso - 2.0 * yza)
    syy = pick(w1 * s[3] + w2 * (exy + eyz), iso + yza + yzb)
    szz = pick(w1 * s[5] + w2 * (exz + eyz), iso + yza - yzb)
    sxy = pick(w2 * mxy, (1.0 / 9.0) * t13)
    syz = pick(w2 * myz, (1.0 / 9.0) * t14)
    sxz = pick(w2 * mxz, (1.0 / 9.0) * t15)
    ux, uy, uz = co["ux"], co["uy"], co["uz"]
    fx, fy, fz = co["fx"], co["fy"], co["fz"]
    vx = sxx * fx + sxy * fy + sxz * fz
    vy = sxy * fx + syy * fy + syz * fz
    vz = sxz * fx + syz * fy + szz * fz
    usq = fx * fx + fy * fy + fz * fz
    phi = (
        s0
        + 3.0 * (s1x * fx + s1y * fy + s1z * fz)
        + 4.5 * (fx * vx + fy * vy + fz * vz)
        - 1.5 * usq * s0
    )
    reff = co["reff"]
    gx = reff * (3.0 * (s1x - fx * s0) + 9.0 * vx)
    gy = reff * (3.0 * (s1y - fy * s0) + 9.0 * vy)
    gz = reff * (3.0 * (s1z - fz * s0) + 9.0 * vz)
    gu = gx * ux + gy * uy + gz * uz
    sens = co["sd"] * gu + co["sk"]
    grho = co["mphi"] * phi - gu * co["r"] + co["kc"]
    rd, hk = co["rd"], co["hk"]
    hx, hy, hz = gx * rd + hk * ux, gy * rd + hk * uy, gz * rd + hk * uz
    mi, evh, odh = co["mi"], co["evh"], co["odh"]
    out = [None] * 19
    out[0] = 2.0 * evh * q[0] - mi * (12.0 * t2 - 30.0 * t1) + grho

    def pair(i, even, odd, ch):
        e = evh * s[i] - mi * even + grho
        o = odh * d[i] - mi * odd + ch
        out[i], out[i + 1] = e + o, e - o

    axis = -11.0 * t1 - 4.0 * t2
    e9 = 2.0 * t10 - t9
    e11 = t11 - 2.0 * t12
    pair(1, axis - 2.0 * e9, -4.0 * t4, hx)
    pair(3, axis + e9 + e11, -4.0 * t6, hy)
    pair(5, axis + e9 - e11, -4.0 * t8, hz)
    edge = 8.0 * t1 + t2
    e910, e112 = t9 + t10, t11 + t12
    bxy, bxz, byz = edge + e910 + e112, edge + e910 - e112, edge - 2.0 * e910
    t4p, t4m = t4 + t16, t4 - t16
    t6m, t6p = t6 - t17, t6 + t17
    t8p, t8m = t8 + t18, t8 - t18
    pair(7, bxy + t13, t4p + t6m, hx + hy)
    pair(9, bxy - t13, t4p - t6m, hx - hy)
    pair(11, bxz + t15, t4m + t8p, hx + hz)
    pair(13, bxz - t15, t4m - t8p, hx - hz)
    pair(15, byz + t14, t6p + t8m, hy + hz)
    pair(17, byz - t14, t6p - t8m, hy - hz)
    return out, sens


SHARED = ("raw", "mi", "evh", "odh", "mphi", "hk", "sd")
PER_STEP = ("ux", "uy", "uz", "fx", "fy", "fz", "reff", "r", "rd", "kc", "sk")


def kernel(
    planes,
    adj_hbm,
    fwd_hbm,
    design_hbm,
    solid_hbm,
    kind_hbm,
    out_ref,
    sens_ref,
    sums_ref,
    av,
    a1,
    fv,
    gv,
    solv,
    kindv,
    shared,
    steps,
    xs,
    zs,
    ys,
    es,
    xr,
    zr,
    dr,
    yr,
    er,
    part,
    zsum,
    line,
    plane,
    load_sem,
    send_sem,
    recv_sem,
    line_send,
    line_recv,
    plane_send,
    plane_recv,
    back_send,
    back_recv,
):
    nz0, ny, ncore, ngy, ngz = planes
    ngx = nz0 * ny * ncore
    iz0, iy, ic = (lax.axis_index(a) for a in GX)
    igy, igz = lax.axis_index("gy"), lax.axis_index("gz")
    me = (iz0 * ny + iy) * ncore + ic
    bx, by, bz = design_hbm.shape

    def device(g, y, z):
        return (
            lax.div(g, ny * ncore),
            lax.rem(lax.div(g, ncore), ny),
            lax.rem(g, ncore),
            y,
            z,
        )

    def target(offset):
        ox, oy, oz = offset
        return device(me + ox, 1 - igy if oy else igy, igz + oz)

    def exists(offset):
        ox, _, oz = offset
        tests = []
        if ox:
            tests.append(me > 0 if ox < 0 else me < ngx - 1)
        if oz:
            tests.append(igz > 0 if oz < 0 else igz < ngz - 1)
        if not tests:
            return None
        return functools.reduce(jnp.logical_and, tests)

    def when(test, action):
        if test is None:
            action()
        else:
            pl.when(test)(action)

    def back(offset):
        return (-offset[0], offset[1], -offset[2])

    loads = [
        (adj_hbm, av),
        (fwd_hbm.at[1], fv.at[1]),
        (design_hbm, gv),
        (solid_hbm, solv),
        (kind_hbm, kindv),
        (fwd_hbm.at[0], fv.at[0]),
    ]
    loads = [
        pltpu.make_async_copy(src, dst, load_sem.at[n])
        for n, (src, dst) in enumerate(loads)
    ]
    for copy in loads:
        copy.start()

    def refs(e, n):
        name = MESSAGES[n][0]
        return {
            "xd": lambda: (xs.at[e, 0], xr.at[e, 0]),
            "xu": lambda: (xs.at[e, 1], xr.at[e, 1]),
            "zd": lambda: (zs.at[e, 0], zr.at[e, 0]),
            "zu": lambda: (zs.at[e, 1], zr.at[e, 1]),
            "dd": lambda: (xs.at[e, 0, 3], dr.at[e, 0]),
            "uu": lambda: (xs.at[e, 1, 3], dr.at[e, 1]),
            "du": lambda: (xs.at[e, 0, 4], dr.at[e, 2]),
            "ud": lambda: (xs.at[e, 1, 4], dr.at[e, 3]),
            "f": lambda: (ys.at[e], yr.at[e]),
            "fxd": lambda: (es.at[e, 0], er.at[e, 0]),
            "fxu": lambda: (es.at[e, 1], er.at[e, 1]),
            "fzd": lambda: (es.at[e, 2], er.at[e, 2]),
            "fzu": lambda: (es.at[e, 3], er.at[e, 3]),
        }[name]()

    def copy_of(e, n):
        src, dst = refs(e, n)
        return pltpu.make_async_remote_copy(
            src_ref=src,
            dst_ref=dst,
            send_sem=send_sem.at[e, n],
            recv_sem=recv_sem.at[e, n],
            device_id=target(MESSAGES[n][1]),
            device_id_type=MESH,
        )

    for e in range(2):
        for n in range(len(MESSAGES)):
            source = exists(back(MESSAGES[n][1]))
            if source is not None:
                dst = refs(e, n)[1]

                def clear(dst=dst):
                    dst[...] = jnp.zeros(dst.shape, f32)

                pl.when(jnp.logical_not(source))(clear)

    barrier = pltpu.get_barrier_semaphore()
    waits = jnp.int32(0)
    for _, offset in MESSAGES:
        test = exists(offset)

        def hello(offset=offset):
            pl.semaphore_signal(
                barrier, inc=1, device_id=target(offset), device_id_type=MESH
            )

        when(test, hello)
        waits = waits + (1 if test is None else test.astype(jnp.int32))
    nz = nz0 * ngy
    z = igy * nz0 + iz0
    nplane = ny * ncore * ngz
    cell = (iy * ncore + ic) * ngz + igz

    def at(zz, p):
        return (
            lax.rem(zz, nz0),
            lax.div(p, ncore * ngz),
            lax.rem(lax.div(p, ngz), ncore),
            lax.div(zz, nz0),
            lax.rem(p, ngz),
        )

    first = z == 0

    @pl.when(first)
    def _():
        def up(i, c):
            pl.semaphore_signal(
                barrier, inc=1, device_id=at(i, cell), device_id_type=MESH
            )
            return c

        lax.fori_loop(1, nz, up, 0)

        def across(i, c):
            peer = lax.rem(cell + i, nplane)
            pl.semaphore_signal(
                barrier, inc=1, device_id=at(0, peer), device_id_type=MESH
            )
            return c

        lax.fori_loop(1, nplane, across, 0)

    @pl.when(jnp.logical_not(first))
    def _():
        pl.semaphore_signal(barrier, inc=1, device_id=at(0, cell), device_id_type=MESH)

    waits = waits + jnp.where(first, nz - 1 + nplane - 1, 1)

    sub = lax.broadcasted_iota(jnp.int32, (by, bz), 0)
    lane = lax.broadcasted_iota(jnp.int32, (by, bz), 1)
    low = igy == 0

    def pack(e, a):
        for n, i in enumerate(X_PLUS):
            xs[e, 0, n] = a[i, 0]
        for n, i in enumerate(X_MINUS):
            xs[e, 1, n] = a[i, bx - 1]

        def faces(pops, row):
            for n, i in enumerate(pops):
                face = a[i, :, row, :]
                ys[e, n] = face
                if n == 1:
                    es[e, 0] = face[0:1]
                if n == 2:
                    es[e, 1] = face[bx - 1 : bx]
                if n in (3, 4):
                    column = face[:, 0:1] if n == 3 else face[:, bz - 1 : bz]
                    spread = jnp.where(lane == sub, column, 0.0)
                    es[e, n - 1] = jnp.sum(spread, axis=0, keepdims=True)

        pl.when(low)(lambda: faces(Y_MINUS, by - 1))
        pl.when(jnp.logical_not(low))(lambda: faces(Y_PLUS, 0))
        for side, (pops, at_lane) in enumerate(((Z_PLUS, 0), (Z_MINUS, bz - 1))):
            packed = jnp.zeros((by, bz), f32)
            for n, i in enumerate(pops):
                for x in range(bx):
                    slot = n * bx + x
                    moved = pltpu.roll(a[i, x], (slot - at_lane) % bz, 1)
                    packed = jnp.where(lane == slot, moved, packed)
            zs[e, side] = packed

    def send(e):
        for n in (*FAR, *NEAR):
            when(exists(MESSAGES[n][1]), lambda n=n: copy_of(e, n).start())

    def receive(e, numbers):
        for n in numbers:
            when(exists(back(MESSAGES[n][1])), lambda n=n: copy_of(e, n).wait_recv())

    def sent(e):
        for n in range(len(MESSAGES)):
            when(exists(MESSAGES[n][1]), lambda n=n: copy_of(e, n).wait_send())

    def precompute(t):
        cost = jnp.zeros((by, bz), f32)
        for x in range(bx):
            g = gv[x]
            fluid = solv[x] == 0
            kind = kindv[x]
            f = [fv[t, i, x] for i in range(19)]
            xpos = (me * bx + x).astype(f32)
            weight = 1.0 + 2.0 * xpos / (ngx * bx - 1)
            fl = fluid.astype(f32)
            damping = (0.1 + g) / (0.5 + 0.6 * g)
            if t == 1:
                inside = jnp.logical_and(fluid, kind == 0).astype(f32)
                put = dict(
                    raw=(kind != 0).astype(f32),
                    mi=inside,
                    evh=0.5 * (inside + 1.0 - fl),
                    odh=0.5 * (inside - 1.0 + fl),
                    mphi=jnp.logical_and(fluid, kind != 2).astype(f32),
                    hk=weight * fl * damping,
                    sd=0.44 / ((0.5 + 0.6 * g) * (0.1 + g)),
                )
                for n, name in enumerate(SHARED):
                    shared[n, x] = put[name]
            axes = []
            for axis in range(3):
                plus = sum(f[i] for i in range(19) if lattice[i, axis] == 1)
                minus = sum(f[i] for i in range(19) if lattice[i, axis] == -1)
                axes.append(plus - minus)
            rho = sum(f)
            r = 1.0 / rho
            rd = r * damping
            ux, uy, uz = (j * rd for j in axes)
            usq = ux * ux + uy * uy + uz * uz
            inlet = kind == 1
            wfu = weight * fl * usq
            reff = jnp.where(kind == 0, rho, jnp.where(kind == 2, 1.0, 0.0)) * fl
            put = dict(
                ux=ux,
                uy=uy,
                uz=uz,
                fx=jnp.where(inlet, 0.08, ux),
                fy=jnp.where(inlet, 0.0, uy),
                fz=jnp.where(inlet, 0.0, uz),
                reff=reff,
                r=r,
                rd=rd,
                kc=-0.5 * wfu,
                sk=shared[SHARED.index("sd"), x] * wfu * rho,
            )
            for n, name in enumerate(PER_STEP):
                steps[t, n, x] = put[name]
            cost = cost + 0.5 * wfu * rho
        return cost

    def pulled_far(e):
        y = [yr[e, n] for n in range(5)]
        rows = [er[e, n] for n in range(4)]
        y[1] = jnp.where(sub == bx - 1, rows[0], pltpu.roll(y[1], bx - 1, 0))
        y[2] = jnp.where(sub == 0, rows[1], pltpu.roll(y[2], 1, 0))
        columns = [
            jnp.sum(jnp.where(lane == sub, rows[n], 0.0), axis=1, keepdims=True)
            for n in (2, 3)
        ]
        y[3] = jnp.where(lane == bz - 1, columns[0], pltpu.roll(y[3], bz - 1, 1))
        y[4] = jnp.where(lane == 0, columns[1], pltpu.roll(y[4], 1, 1))
        return y

    def near(e, a, i, x):
        cx, cy, cz = (int(v) for v in lattice[i])
        xx = x + cx
        inside = 0 <= xx < bx
        if inside:
            tile = a[i, xx]
        else:
            tile = xr[e, 0, X_PLUS.index(i)] if cx > 0 else xr[e, 1, X_MINUS.index(i)]
        if cz == 0:
            return tile
        if inside:
            pops = Z_PLUS if cz > 0 else Z_MINUS
            slot = pops.index(i) * bx + xx
            halo = pltpu.roll(
                zr[e, 0 if cz > 0 else 1], ((bz - 1 if cz > 0 else 0) - slot) % bz, 1
            )
        else:
            halo = dr[e, {11: 0, 12: 1, 13: 2, 14: 3}[i]]
            halo = pltpu.roll(halo, (bz - 1) if cz > 0 else 1, 1)
        moved = pltpu.roll(tile, (bz - 1) if cz > 0 else 1, 1)
        return jnp.where(lane == (bz - 1 if cz > 0 else 0), halo, moved)

    def step(e, a, t, write):
        total = jnp.zeros((by, bz), f32)
        far = pulled_far(e)
        up = [jnp.where(low, v, 0.0) for v in far]
        down = [jnp.where(low, 0.0, v) for v in far]
        for x in range(bx):
            q = []
            for i in range(19):
                tile = near(e, a, i, x)
                cy = int(lattice[i, 1])
                if cy > 0:
                    row = up[Y_PLUS.index(i)][x : x + 1]
                    tile = jnp.where(sub == by - 1, row, pltpu.roll(tile, by - 1, 0))
                elif cy < 0:
                    row = down[Y_MINUS.index(i)][x : x + 1]
                    tile = jnp.where(sub == 0, row, pltpu.roll(tile, 1, 0))
                q.append(tile)
            co = {name: shared[n, x] for n, name in enumerate(SHARED)}
            co.update({name: steps[t, n, x] for n, name in enumerate(PER_STEP)})
            out, sens = step_tile(q, co)
            write(x, out, sens)

    loads[0].wait()
    pack(0, av)
    pl.semaphore_wait(barrier, waits)
    send(0)
    for copy in loads[1:]:
        copy.wait()
    cost = precompute(1) + precompute(0)
    receive(0, NEAR)
    receive(0, FAR)

    def write_first(x, out, sens):
        for i in range(19):
            a1[i, x] = out[i]
        sens_ref[x] = sens

    step(0, av, 1, write_first)
    pack(1, a1)
    send(1)
    receive(1, NEAR)
    receive(1, FAR)
    squares = []

    def write_second(x, out, sens):
        for i in range(19):
            out_ref[i, x] = out[i]
        both = sens_ref[x] + sens
        sens_ref[x] = both
        squares.append(both * both)

    step(1, a1, 0, write_second)
    square = functools.reduce(jnp.add, squares)
    part[0:1] = jnp.sum(square, axis=0, keepdims=True)
    part[1:2] = jnp.sum(cost, axis=0, keepdims=True)

    @pl.when(jnp.logical_not(first))
    def _():
        up = pltpu.make_async_remote_copy(
            src_ref=part,
            dst_ref=line.at[z],
            send_sem=line_send,
            recv_sem=line_recv.at[z],
            device_id=at(0, cell),
            device_id_type=MESH,
        )
        up.start()
        up.wait_send()

    @pl.when(first)
    def _():
        total = part[...]
        for i in range(1, nz):
            pltpu.make_async_remote_copy(
                src_ref=part,
                dst_ref=line.at[i],
                send_sem=line_send,
                recv_sem=line_recv.at[i],
                device_id=at(i, cell),
                device_id_type=MESH,
            ).wait_recv()
        for i in range(1, nz):
            total = total + line[i]
        zsum[...] = total
        plane[cell] = total

        def out(i, c):
            peer = lax.rem(cell + i, nplane)
            pltpu.make_async_remote_copy(
                src_ref=zsum,
                dst_ref=plane.at[cell],
                send_sem=plane_send.at[peer],
                recv_sem=plane_recv.at[cell],
                device_id=at(0, peer),
                device_id_type=MESH,
            ).start()
            return c

        lax.fori_loop(1, nplane, out, 0)

        def arrived(i, c):
            peer = lax.rem(cell + i, nplane)
            copy = pltpu.make_async_remote_copy(
                src_ref=zsum,
                dst_ref=plane.at[peer],
                send_sem=plane_send.at[peer],
                recv_sem=plane_recv.at[peer],
                device_id=at(0, peer),
                device_id_type=MESH,
            )
            copy.wait_recv()
            copy.wait_send()
            return c

        lax.fori_loop(1, nplane, arrived, 0)
        parts = [plane[i] for i in range(nplane)]
        while len(parts) > 1:
            parts = [a + b for a, b in zip(parts[::2], parts[1::2])]
        sums_ref[...] = parts[0]

        def down(i, c):
            pltpu.make_async_remote_copy(
                src_ref=sums_ref,
                dst_ref=sums_ref,
                send_sem=back_send.at[i],
                recv_sem=back_recv,
                device_id=at(i, cell),
                device_id_type=MESH,
            ).start()
            return c

        lax.fori_loop(1, nz, down, 0)

        def gone(i, c):
            pltpu.make_async_remote_copy(
                src_ref=sums_ref,
                dst_ref=sums_ref,
                send_sem=back_send.at[i],
                recv_sem=back_recv,
                device_id=at(i, cell),
                device_id_type=MESH,
            ).wait_send()
            return c

        lax.fori_loop(1, nz, gone, 0)

    @pl.when(jnp.logical_not(first))
    def _():
        pltpu.make_async_remote_copy(
            src_ref=sums_ref,
            dst_ref=sums_ref,
            send_sem=back_send.at[0],
            recv_sem=back_recv,
            device_id=at(0, cell),
            device_id_type=MESH,
        ).wait_recv()

    sent(0)
    sent(1)


def finish_kernel(cells, adj, sens, sums, adj_out, sens_out, scal_out, buf, sems):
    copy = pltpu.make_async_copy(adj, adj_out, sems.at[0])
    copy.start()
    totals = jnp.sum(sums[...], axis=1, keepdims=True)
    rms = jnp.sqrt(totals[0:1] / cells + 1e-06)
    objective = totals[1:2] / cells
    buf[...] = sens[...] / rms[None]
    copy2 = pltpu.make_async_copy(buf, sens_out, sems.at[1])
    copy2.start()
    scal_out[0:1] = jnp.broadcast_to(objective, (1, 128))
    scal_out[1:2] = jnp.broadcast_to(rms, (1, 128))
    copy.wait()
    copy2.wait()


def body(planes, adjoint_in, forward_states, design, solid_mask, boundary_kind):
    nz0, ny, ncore, ngy, ngz = planes
    bx, by, bz = design.shape
    nz, nplane = nz0 * ngy, ny * ncore * ngz
    vmem = pl.BlockSpec(memory_space=pltpu.VMEM)
    hbm = pl.BlockSpec(memory_space=pl.ANY)
    dma = pltpu.SemaphoreType.DMA
    n = len(MESSAGES)
    adj, sens, sums = pl.pallas_call(
        functools.partial(kernel, planes),
        out_shape=(
            jax.ShapeDtypeStruct(adjoint_in.shape, f32),
            jax.ShapeDtypeStruct(design.shape, f32),
            jax.ShapeDtypeStruct((2, bz), f32),
        ),
        in_specs=[hbm] * 5,
        out_specs=(vmem, vmem, vmem),
        scratch_shapes=[
            pltpu.VMEM(adjoint_in.shape, f32),
            pltpu.VMEM(adjoint_in.shape, f32),
            pltpu.VMEM(forward_states.shape, f32),
            pltpu.VMEM(design.shape, f32),
            pltpu.VMEM(design.shape, jnp.int32),
            pltpu.VMEM(design.shape, jnp.int32),
            pltpu.VMEM((len(SHARED), bx, by, bz), f32),
            pltpu.VMEM((2, len(PER_STEP), bx, by, bz), f32),
            pltpu.VMEM((2, 2, 5, by, bz), f32),
            pltpu.VMEM((2, 2, by, bz), f32),
            pltpu.VMEM((2, 5, bx, bz), f32),
            pltpu.VMEM((2, 4, 1, bz), f32),
            pltpu.VMEM((2, 2, 5, by, bz), f32),
            pltpu.VMEM((2, 2, by, bz), f32),
            pltpu.VMEM((2, 4, by, bz), f32),
            pltpu.VMEM((2, 5, bx, bz), f32),
            pltpu.VMEM((2, 4, 1, bz), f32),
            pltpu.VMEM((2, bz), f32),
            pltpu.VMEM((2, bz), f32),
            pltpu.VMEM((nz, 2, bz), f32),
            pltpu.VMEM((nplane, 2, bz), f32),
            dma((6,)),
            dma((2, n)),
            dma((2, n)),
            dma,
            dma((nz,)),
            dma((nplane,)),
            dma((nplane,)),
            dma((nz,)),
            dma,
        ],
        compiler_params=pltpu.CompilerParams(collective_id=0, has_side_effects=True),
        name="adjoint_steps",
    )(adjoint_in, forward_states, design, solid_mask, boundary_kind)
    cells = float(nz0 * ny * ncore * bx * ngy * by * ngz * bz)
    adjoint, sensitivity, scalars = pl.pallas_call(
        functools.partial(finish_kernel, cells),
        out_shape=(
            jax.ShapeDtypeStruct(adjoint_in.shape, f32),
            jax.ShapeDtypeStruct(design.shape, f32),
            jax.ShapeDtypeStruct((2, 128), f32),
        ),
        in_specs=[vmem, vmem, vmem],
        out_specs=(hbm, hbm, vmem),
        scratch_shapes=[pltpu.VMEM(design.shape, f32), dma((2,))],
        name="finish",
    )(adj, sens, sums)
    return adjoint, sensitivity, scalars[0, 0], scalars[1, 0]


def solution(mesh):
    ngy, ngz = mesh.shape["gy"], mesh.shape["gz"]
    planes = (6, 8, 2, ngy, ngz)
    torus = Mesh(mesh.devices.reshape(planes), AXES)
    placed = (
        P(None, GX, "gy", "gz"),
        P(None, None, GX, "gy", "gz"),
        P(GX, "gy", "gz"),
        P(GX, "gy", "gz"),
        P(GX, "gy", "gz"),
    )
    return jax.shard_map(
        functools.partial(body, planes),
        mesh=torus,
        in_specs=placed,
        out_specs=(P(None, GX, "gy", "gz"), P(GX, "gy", "gz"), P(), P()),
        check_vma=False,
    )
```
